32 devices in a mesh: dp: 16 (over z, x, core), head: 2 (over y).
Axes of the slice: x: 2, y: 2, z: 4, core: 2. Of those that a mesh axis runs over, the one named last changes fastest.
Arguments:
- features: bfloat16 [2, 32, 196, 1024], P(None, ('dp', 'head'))
- patch_mask: int32 [2, 32, 196], P(None, ('dp', 'head')), may hold values from 0 to 1, as said below
- w_first: bfloat16 [1024, 2048], P('dp'), may hold values from -0.1875 to 0.1875
- w_second: bfloat16 [2048, 256], P('dp'), may hold values from -0.125 to 0.125
- proto_weight: bfloat16 [256, 8192], P('dp', 'head'), may hold values from -6 to 6
- center: float32 [8192], replicated, may hold values from -0.04 to 0.04
Outputs:
- targets: bfloat16 [2, 3136, 8192], P(None, ('dp', 'head'))
- new_center: float32 [8192], P('head')
The draws below stay inside these ranges and needn't reach their ends.
Inputs may be any that keep to these rules, and one draw needn't show every extreme that they name: `patch_mask`: in each view every image masks between 19 and 98 of its patches, so that a block of 1 images fills at most 98 slots; in every draw the images of some block fill all 98 slots.
All inputs are finite; a program needn't handle non-finite values.
Results may differ from the reference program's by a relative error of at most 0.0086.
Values may be sent and summed in bfloat16 or wider, within the bound.
No kernel may reach another device: no remote copies, remote signals or barrier semaphores. Data moves between devices by JAX's collectives and lax.ppermute only.
A program may use at most 64 MiB of HBM per device.

```python
import jax
import jax.numpy as jnp
from jax import lax

D = 1024
HID = 2048
BOT = 256
PROTO = 8192
PATCH = 196
VIEWS = 2
IMG_DEV = 1
MAXMASK = 98
CAP = 98
IMAGES = 32
SLOTS = 3136
N_DP = 16
N_HEAD = 2


def draw_features(key, part):
    key = jax.random.fold_in(key, 11)
    k_noise, k_first, k_second = jax.random.split(key, 3)
    shape = (VIEWS, IMAGES, PATCH, D)
    along = (jnp.arange(IMAGES, dtype=jnp.float32) / IMAGES).reshape(1, IMAGES, 1, 1)
    first = jax.random.normal(k_first, (VIEWS, 1, 1, D), jnp.float32)
    second = jax.random.normal(k_second, (VIEWS, 1, 1, D), jnp.float32)
    noise = jax.random.normal(k_noise, shape, jnp.float32)
    values = noise + 0.7 * first + 1.4 * along * second
    return values.astype(jnp.bfloat16)


def draw_patch_mask(key, part):
    key = jax.random.fold_in(key, 23)
    k_count, k_order, k_full = jax.random.split(key, 3)
    image = jnp.arange(IMAGES, dtype=jnp.int32)
    lowest = PATCH // 10 + PATCH * 4 // 10 * image // IMAGES
    counts = jax.random.randint(k_count, (VIEWS, IMAGES), 0, PATCH // 10 + 1, dtype=jnp.int32) + lowest[None, :]
    counts = jnp.minimum(counts, MAXMASK)
    full_block = jax.random.randint(k_full, (), 0, IMAGES // IMG_DEV, dtype=jnp.int32)
    counts = jnp.where((image // IMG_DEV == full_block)[None, :], MAXMASK, counts)
    scores = jax.random.randint(k_order, (VIEWS, IMAGES, PATCH), 0, 1 << 20, dtype=jnp.int32) * PATCH + jnp.arange(PATCH, dtype=jnp.int32)
    ranks = jnp.argsort(jnp.argsort(scores, axis=-1, stable=True), axis=-1, stable=True).astype(jnp.int32)
    return (ranks < counts[:, :, None]).astype(jnp.int32)


def levels(own_key, extent, cuts, smallest, top_value):
    factor_of, own = 1.0, jax.random.fold_in(own_key, 6)
    for axis_at, blocks in cuts:
        heights = jnp.exp(jax.random.uniform(jax.random.fold_in(own, axis_at), (blocks,), jnp.float32, smallest / len(cuts), top_value / len(cuts)))
        factor_of = factor_of * jnp.repeat(heights, extent[axis_at] // blocks).reshape([-1 if axis == axis_at else 1 for axis in range(len(extent))])
    return factor_of


def bell_draw(stream_key, extent, scale, reach, shards=(), kind=jnp.bfloat16):
    loudness = levels(stream_key, extent, shards, -0.22, 0.18) if shards else 1.0
    array = jax.random.normal(stream_key, extent, jnp.float32) * scale * loudness
    return jnp.minimum(jnp.maximum(array, -reach), reach).astype(kind)


def setup_inputs(seed: int = 0) -> dict:
    key_list = jax.random.split(jax.random.key(seed), 7)
    features = draw_features(jax.random.fold_in(key_list[6], 71), 0)
    patch_mask = draw_patch_mask(jax.random.fold_in(key_list[6], 71), 0)
    w_first = bell_draw(key_list[2], (D, HID), D ** -0.5, 0.1875, ((0, 16),))
    w_second = bell_draw(key_list[3], (HID, BOT), HID ** -0.5, 0.125, ((0, 16),))
    proto_weight = bell_draw(key_list[4], (BOT, PROTO), 1.0, 6.0, ((0, 16), (1, 2)))
    center = bell_draw(key_list[5], (PROTO,), 0.01, 0.04, (), jnp.float32)
    return dict(features=features, patch_mask=patch_mask, w_first=w_first, w_second=w_second, proto_weight=proto_weight, center=center)


teacher_temp = 0.04
center_momentum = 0.9

def pack_block(block_feats, block_mask):
    flat_mask = block_mask.reshape(-1)
    flat_feats = block_feats.reshape(-1, block_feats.shape[-1])
    places = jnp.nonzero(flat_mask, size=CAP, fill_value=0)[0].astype(jnp.int32)
    live = jnp.arange(CAP, dtype=jnp.int32) < jnp.sum(flat_mask).astype(jnp.int32)
    rows = jnp.where(live[:, None], flat_feats[places], jnp.zeros((), flat_feats.dtype))
    return (rows, live)

def bottleneck(rows, w_first, w_second):
    hidden = jax.nn.gelu(jnp.dot(rows, w_first, preferred_element_type=jnp.float32), approximate=False).astype(jnp.bfloat16)
    projected = jnp.dot(hidden, w_second, preferred_element_type=jnp.float32)
    scale = lax.rsqrt(lax.optimization_barrier(jnp.sum(projected * projected, axis=-1, keepdims=True)) + 1e-06)
    return (projected * scale).astype(jnp.bfloat16)

def reference(features, patch_mask, w_first, w_second, proto_weight, center):
    blocks = N_DP * N_HEAD
    feats = features.reshape(VIEWS, blocks, IMG_DEV * PATCH, D)
    masks = patch_mask.reshape(VIEWS, blocks, IMG_DEV * PATCH)
    columns = proto_weight.astype(jnp.float32)
    unit_protos = (columns * lax.rsqrt(lax.optimization_barrier(jnp.sum(columns * columns, axis=0, keepdims=True)) + 1e-06)).astype(jnp.bfloat16)
    outputs = []
    current = center
    for view in range(VIEWS):

        def one_block(pair, current=current):
            rows, live = pack_block(pair[0], pair[1])
            normed = bottleneck(rows, w_first, w_second)
            logits = jnp.dot(normed, unit_protos, preferred_element_type=jnp.float32)
            exps = jnp.exp((logits - current) / teacher_temp)
            probs = PROTO * exps / lax.optimization_barrier(jnp.sum(exps, axis=1, keepdims=True))
            targets = jnp.where(live[:, None], probs, jnp.zeros((), jnp.float32)).astype(jnp.bfloat16)
            return (targets, lax.optimization_barrier(jnp.sum(logits, axis=0)), jnp.sum(live.astype(jnp.float32)))
        targets, partials, counts = lax.map(one_block, (feats[view], masks[view]))
        outputs.append(targets.reshape(SLOTS, PROTO))
        current = center_momentum * current + (1.0 - center_momentum) * lax.optimization_barrier(jnp.sum(partials, axis=0)) / jnp.sum(counts)
    return (jnp.stack(outputs), current)
```

```python
import functools

import jax
import jax.numpy as jnp
from jax import lax
from jax.experimental import pallas as pl
from jax.experimental.pallas import tpu as pltpu
from jax.sharding import PartitionSpec as P

teacher_temp = 0.04
center_momentum = 0.9
VMEM = pl.BlockSpec(memory_space=pltpu.VMEM)
HBM = pl.BlockSpec(memory_space=pl.ANY)
SPLIT = 3


def hop(x, axis, mask):
    size = lax.axis_size(axis)
    return lax.ppermute(x, axis, [(i, i ^ mask) for i in range(size)])


def round_up(n, m):
    return -(-n // m) * m


def pack_kernel(slots, feats_ref, mask_ref, rows_ref):
    views, patches, width = feats_ref.shape
    before = lax.broadcasted_iota(jnp.int32, (patches, patches), 0)
    after = lax.broadcasted_iota(jnp.int32, (patches, patches), 1)
    upto = (before <= after).astype(jnp.bfloat16)
    slot = lax.broadcasted_iota(jnp.int32, (slots, patches), 0)
    packed = []
    for view in range(views):
        mask = mask_ref[view]
        marks = jnp.broadcast_to(mask, (16, patches)).astype(jnp.float32).astype(jnp.bfloat16)
        rank = jnp.dot(marks, upto, preferred_element_type=jnp.float32)[0:1].astype(jnp.int32)
        wanted = jnp.where(mask > 0, rank - 1, -1)
        pick = (slot == wanted).astype(jnp.float32).astype(jnp.bfloat16)
        packed.append(jnp.dot(pick, feats_ref[view], preferred_element_type=jnp.float32))
    rows_ref[...] = jnp.concatenate(packed, axis=0).astype(jnp.bfloat16)


def pack_rows(features, patch_mask, slots):
    views, images, patches, width = features.shape
    feats = features.reshape(views, images * patches, width)
    mask = patch_mask.reshape(views, 1, images * patches)
    return pl.pallas_call(
        functools.partial(pack_kernel, slots),
        out_shape=jax.ShapeDtypeStruct((views * slots, width), jnp.bfloat16),
        in_specs=[VMEM, VMEM],
        out_specs=VMEM,
        name="pack_rows",
    )(feats, mask)


def spread_far(x, size):
    bits = []
    bit = 4
    while bit < size:
        bits.append(bit)
        bit *= 2
    current, masks = x, [0]
    for bit in bits[:-1]:
        current = jnp.concatenate([current, hop(current, "dp", bit)], axis=0)
        masks = masks + [m ^ bit for m in masks]
    pieces = [(current, masks)]
    for bit in bits[-1:]:
        pieces.append((hop(current, "dp", bit), [m ^ bit for m in masks]))
    return pieces


def spread(pieces, axis, bit):
    return pieces + [(hop(x, axis, bit), [m ^ bit for m in masks]) for x, masks in pieces]


def in_order(pieces, rows):
    blocks = [x[i * rows : (i + 1) * rows] for x, masks in pieces for i in range(len(masks))]
    masks = [m for _, ms in pieces for m in ms]
    place = jnp.asarray([masks.index(m) for m in range(len(masks))], jnp.int32)
    me = lax.axis_index("dp")
    order = jnp.take(place, jnp.arange(len(masks), dtype=jnp.int32) ^ me)
    return jnp.take(jnp.stack(blocks), order, axis=0).reshape(-1, blocks[0].shape[1])


def load_blocks(refs, plan, rows, target, sem):
    me = lax.axis_index("dp")
    head = lax.axis_index("head")
    copies = []
    for ref, (masks, head_mask) in zip(refs, plan):
        wide = ref.shape[1]
        left = 0 if head_mask is None else pl.multiple_of((head ^ head_mask) * wide, wide)
        if masks is None:
            copies.append(
                pltpu.make_async_copy(ref, target.at[:, pl.ds(left, wide)], sem)
            )
            continue
        for i, m in enumerate(masks):
            top = pl.multiple_of((me ^ m) * rows, rows)
            copies.append(
                pltpu.make_async_copy(
                    ref.at[pl.ds(i * rows, rows), :],
                    target.at[pl.ds(top, rows), pl.ds(left, wide)],
                    sem,
                )
            )
    return copies


def layers_kernel(plan, block, width, bottle, *refs):
    own_ref, far_ref = refs[:2]
    piece_refs = refs[2 : 2 + len(plan)]
    mine_ref, theirs_ref, weights, sem = refs[2 + len(plan) :]
    copies = load_blocks(piece_refs, plan, block, weights, sem)
    for copy in copies:
        copy.start()
    rows = jnp.concatenate([own_ref[...], far_ref[...]], axis=0)
    for copy in copies:
        copy.wait()
    hidden_width = weights.shape[1] - bottle
    step = min(256, hidden_width)
    total = jnp.zeros((rows.shape[0], bottle), jnp.float32)
    for i in range(hidden_width // step):
        pre = jnp.dot(rows, weights[:, i * step : (i + 1) * step], preferred_element_type=jnp.float32)
        hidden = (0.5 * pre * (1.0 + lax.erf(pre * (0.5**0.5)))).astype(jnp.bfloat16)
        total += jnp.dot(
            hidden, weights[i * step : (i + 1) * step, hidden_width:], preferred_element_type=jnp.float32
        )
    count = own_ref.shape[0]
    mine_ref[...] = total[:count]
    theirs_ref[...] = total[count:]


def layers(own, far, pieces, block, bottle):
    plan = [(masks, None) for _, masks in pieces]
    height = block * sum(len(masks) for masks, _ in plan)
    wide = pieces[0][0].shape[1]
    part = jax.ShapeDtypeStruct((own.shape[0], bottle), jnp.float32)
    return pl.pallas_call(
        functools.partial(layers_kernel, plan, block, own.shape[1], bottle),
        out_shape=(part, part),
        in_specs=[VMEM, VMEM] + [HBM] * len(plan),
        out_specs=(VMEM, VMEM),
        scratch_shapes=[pltpu.VMEM((height, wide), jnp.bfloat16), pltpu.SemaphoreType.DMA],
        name="layers",
    )(own, far, *[x for x, _ in pieces])


def norm_kernel(views, mine_ref, got_ref, mask_ref, normed_ref, sums_ref):
    projected = mine_ref[...] + got_ref[...]
    scale = lax.rsqrt(jnp.sum(projected * projected, axis=-1, keepdims=True) + 1e-06)
    normed = (projected * scale).astype(jnp.bfloat16)
    normed_ref[...] = normed
    slots = normed.shape[0] // views
    exact = normed.astype(jnp.float32)
    bottle = normed.shape[1]
    lines = [jnp.sum(exact[v * slots : (v + 1) * slots], axis=0, keepdims=True) for v in range(views)]
    for v in range(views):
        count = jnp.sum(mask_ref[v].astype(jnp.float32), axis=1, keepdims=True)
        lines.append(jnp.broadcast_to(count, (1, bottle)))
    lines.append(jnp.zeros((sums_ref.shape[0] - len(lines), bottle), jnp.float32))
    sums_ref[...] = jnp.concatenate(lines, axis=0)


def norm_rows(mine, got, mask, views):
    return pl.pallas_call(
        functools.partial(norm_kernel, views),
        out_shape=(
            jax.ShapeDtypeStruct(mine.shape, jnp.bfloat16),
            jax.ShapeDtypeStruct((round_up(2 * views, 8), mine.shape[1]), jnp.float32),
        ),
        in_specs=[VMEM, VMEM, VMEM],
        out_specs=(VMEM, VMEM),
        name="norm_rows",
    )(mine, got, mask)


def target_kernel(plan, block, views, capacity, *refs):
    normed_ref, sums_ref, mask_ref, center_ref = refs[:4]
    piece_refs = refs[4 : 4 + len(plan)]
    out_ref, new_ref, protos, exps, lhs, ready, sem, out_sem = refs[4 + len(plan) :]
    copies = load_blocks(piece_refs, plan, block, protos, sem)
    for copy in copies:
        copy.start()
    rows = normed_ref.shape[0]
    slots = rows // views
    bottle, total = protos.shape
    lhs[:rows] = normed_ref[...].astype(jnp.float32)
    rest = sums_ref[0:views]
    parts = []
    for _ in range(SPLIT):
        part = rest.astype(jnp.bfloat16).astype(jnp.float32)
        parts.append(part)
        rest = rest - part
    parts.append(jnp.zeros((lhs.shape[0] - rows - SPLIT * views, bottle), jnp.float32))
    lhs[rows:] = jnp.concatenate(parts, axis=0)
    left = lhs[...].astype(jnp.bfloat16)
    counts = [sums_ref[views + v : views + v + 1, 0:1] for v in range(views)]
    for copy in copies:
        copy.wait()
    step = min(1024, total)
    row_sums = [jnp.zeros((slots, 1), jnp.float32) for _ in range(views)]
    for i in range(total // step):
        cols = slice(i * step, (i + 1) * step)
        weights = protos[:, cols]
        exact = weights.astype(jnp.float32)
        scale = lax.rsqrt(jnp.sum(exact * exact, axis=0, keepdims=True) + 1e-06)
        logits = jnp.dot(left, weights, preferred_element_type=jnp.float32) * scale
        center = center_ref[:, cols]
        for v in range(views):
            e = jnp.exp((logits[v * slots : (v + 1) * slots] - center) * (1.0 / teacher_temp))
            exps[v * slots : (v + 1) * slots, cols] = e
            row_sums[v] += jnp.sum(e, axis=1, keepdims=True)
            sums = sum(logits[rows + k * views + v : rows + k * views + v + 1] for k in range(SPLIT))
            center = center_momentum * center + (1.0 - center_momentum) * sums / counts[v]
        new_ref[:, cols] = center
    slot = lax.broadcasted_iota(jnp.int32, (slots, 1), 0)
    gains = []
    for v in range(views):
        live = jnp.sum(mask_ref[v], axis=1, keepdims=True)
        gains.append(jnp.where(slot < live, total / row_sums[v], 0.0))
    outs = []
    for v in range(views):
        for i in range(total // step):
            cols = slice(i * step, (i + 1) * step)
            ready[v, :, cols] = (exps[v * slots : (v + 1) * slots, cols] * gains[v])[:capacity].astype(jnp.bfloat16)
            copy = pltpu.make_async_copy(ready.at[v, :, cols], out_ref.at[v, :, cols], out_sem)
            copy.start()
            outs.append(copy)
    for copy in outs:
        copy.wait()


def targets_of(normed, sums, mask, center, pieces, block, views, capacity, total):
    plan = [(masks, head_mask) for _, masks, head_mask in pieces]
    bottle = normed.shape[1]
    rows = normed.shape[0]
    return pl.pallas_call(
        functools.partial(target_kernel, plan, block, views, capacity),
        out_shape=(
            jax.ShapeDtypeStruct((views, capacity, total), jnp.bfloat16),
            jax.ShapeDtypeStruct((1, total), jnp.float32),
        ),
        in_specs=[VMEM] * 4 + [HBM] * len(plan),
        out_specs=(HBM, VMEM),
        scratch_shapes=[
            pltpu.VMEM((bottle, total), jnp.bfloat16),
            pltpu.VMEM((rows, total), jnp.float32),
            pltpu.VMEM((round_up(rows + SPLIT * views, 16), bottle), jnp.float32),
            pltpu.VMEM((views, capacity, total), jnp.bfloat16),
            pltpu.SemaphoreType.DMA,
            pltpu.SemaphoreType.DMA,
        ],
        compiler_params=pltpu.CompilerParams(vmem_limit_bytes=48 * 1024 * 1024),
        name="targets",
    )(normed, sums, mask, center.reshape(1, total), *[x for x, _, _ in pieces])


def shards(features, patch_mask, w_first, w_second, proto_weight, center):
    n_dp = lax.axis_size("dp")
    n_head = lax.axis_size("head")
    me = lax.axis_index("dp")
    head = lax.axis_index("head")
    views, images, patches, width = features.shape
    capacity = images * (patches // 2)
    slots = round_up(capacity, 8)
    bottle = w_second.shape[1]
    mask = patch_mask.reshape(views, 1, images * patches)

    core = me & 1
    side = head & 1
    depth, hidden = w_first.shape
    share = w_second.shape[0]
    half = share // 2
    kept = lax.dynamic_slice_in_dim(w_second, core * half, half, 0)
    given = lax.dynamic_slice_in_dim(w_second, (1 - core) * half, half, 0)
    second = jnp.where(core == side, kept, hop(given, "dp", 1))
    first = lax.dynamic_index_in_dim(w_first.reshape(depth, n_dp // 2, 2, share), side, 2, keepdims=False)
    weight = jnp.concatenate([first.reshape(depth, hidden // 2), second.reshape(depth, half * bottle // depth)], axis=1)

    rows = pack_rows(features, patch_mask, slots)
    far_rows = hop(rows, "head", 1)

    weights = spread(spread(spread_far(weight, n_dp), "dp", 2), "dp", 1)
    mine, theirs = layers(rows, far_rows, weights, depth, bottle)
    normed, sums = norm_rows(mine, hop(theirs, "head", 1), mask, views)

    bit = 1
    while bit < n_dp:
        sums = sums + hop(sums, "dp", bit)
        bit *= 2
    bit = 1
    while bit < n_head:
        sums = sums + hop(sums, "head", bit)
        bit *= 2

    block, share_protos = proto_weight.shape
    near = spread(spread_far(proto_weight, n_dp), "dp", 2)
    pieces = [(x, masks, 0) for x, masks in near]
    bit = 1
    while bit < n_head:
        pieces += [(hop(x, "head", bit), masks, h ^ bit) for x, masks, h in pieces]
        bit *= 2
    pieces += [(hop(x, "dp", 1), [m ^ 1 for m in masks], h) for x, masks, h in pieces]
    if block % 16:
        by_head = {}
        for x, masks, h in pieces:
            by_head.setdefault(h, []).append((x, masks))
        pieces = [(in_order(parts, block), None, h) for h, parts in by_head.items()]
    targets, latest = targets_of(
        normed, sums, mask, center, pieces, block, views, capacity, share_protos * n_head
    )
    new_center = lax.dynamic_slice_in_dim(latest[0], head * share_protos, share_protos, 0)
    return (targets, new_center)


def solution(mesh):
    placed = (
        P(None, ("dp", "head"), None, None),
        P(None, ("dp", "head"), None),
        P("dp", None),
        P("dp", None),
        P("dp", "head"),
        P(),
    )
    return jax.shard_map(
        shards,
        mesh=mesh,
        in_specs=placed,
        out_specs=(P(None, ("dp", "head"), None), P("head")),
        check_vma=False,
    )
```

```python
import functools

import jax
import jax.numpy as jnp
from jax import lax
from jax.experimental import pallas as pl
from jax.experimental.pallas import tpu as pltpu
from jax.sharding import PartitionSpec as P


teacher_temp = 0.04
center_momentum = 0.9
VMEM = pl.BlockSpec(memory_space=pltpu.VMEM)
HBM = pl.BlockSpec(memory_space=pl.ANY)
SPLIT = 3
MIB = 1024 * 1024
LANES = 128


def room(mib):
    return pltpu.CompilerParams(vmem_limit_bytes=mib * MIB)


def hop(x, axis, mask):
    size = lax.axis_size(axis)
    return lax.ppermute(x, axis, [(i, i ^ mask) for i in range(size)])


def round_up(n, m):
    return -(-n // m) * m


def by_mask(source, shift, out):
    low = lax.broadcasted_iota(jnp.int32, (LANES, LANES), 0)
    high = lax.broadcasted_iota(jnp.int32, (LANES, LANES), 1)
    within = (low == (high ^ (shift % LANES))).astype(jnp.float32).astype(jnp.bfloat16)
    for t in range(out.shape[1] // LANES):
        start = pl.multiple_of((t ^ (shift // LANES)) * LANES, LANES)
        tile = source[:, pl.ds(start, LANES)].astype(jnp.bfloat16)
        moved = jnp.dot(tile, within, preferred_element_type=jnp.float32)
        out[:, t * LANES : (t + 1) * LANES] = moved.astype(out.dtype)


def pack_kernel(depth, feats_ref, mask_ref, rows_ref, found):
    patches, views, width = feats_ref.shape
    lines = patches * views
    patch = lax.broadcasted_iota(jnp.int32, (patches, lines), 0)
    line = lax.broadcasted_iota(jnp.int32, (patches, lines), 1)
    upto = (patch * views <= line).astype(jnp.float32).astype(jnp.bfloat16)
    same = (patch == line // views).astype(jnp.float32).astype(jnp.bfloat16)
    marks = jnp.concatenate([mask_ref[v].astype(jnp.float32) for v in range(views)], axis=0)
    marks = jnp.concatenate([marks, jnp.zeros((16 - views, patches), jnp.float32)], axis=0).astype(jnp.bfloat16)
    rank = jnp.dot(marks, upto, preferred_element_type=jnp.float32).astype(jnp.int32)
    hit = jnp.dot(marks, same, preferred_element_type=jnp.float32)
    at = lax.broadcasted_iota(jnp.int32, (1, lines), 1)
    key = jnp.full((1, lines), -1, jnp.int32)
    for v in range(views):
        wanted = (at % views == v) & (hit[v : v + 1] > 0.5)
        key = jnp.where(wanted, (rank[v : v + 1] - 1) * views + v, key)
    slot = lax.broadcasted_iota(jnp.int32, (rows_ref.shape[0], lines), 0)
    pick = (slot == key).astype(jnp.float32).astype(jnp.bfloat16)
    feats = feats_ref[...].reshape(lines, width)
    found[...] = jnp.dot(pick, feats, preferred_element_type=jnp.float32)
    by_mask(found, lax.axis_index("dp") * depth, rows_ref)


def pack_rows(features, patch_mask, slots, depth):
    views, images, patches, width = features.shape
    feats = features.reshape(views, images * patches, width).transpose(1, 0, 2)
    mask = patch_mask.reshape(views, 1, images * patches)
    return pl.pallas_call(
        functools.partial(pack_kernel, depth),
        out_shape=jax.ShapeDtypeStruct((views * slots, width), jnp.bfloat16),
        in_specs=[VMEM, VMEM],
        out_specs=VMEM,
        scratch_shapes=[pltpu.VMEM((views * slots, width), jnp.float32)],
        compiler_params=room(16),
        name="pack_rows",
    )(feats, mask)


def prep_kernel(share, first_ref, second_ref, out_ref):
    side = lax.axis_index("head") % 2
    half = share // 2
    hidden = first_ref.shape[1]
    for k in range(hidden // (2 * share)):
        low = first_ref[:, 2 * k * share : (2 * k + 1) * share].astype(jnp.float32)
        high = first_ref[:, (2 * k + 1) * share : (2 * k + 2) * share].astype(jnp.float32)
        even = jnp.concatenate([low[:, :half], high[:, :half]], axis=1)
        odd = jnp.concatenate([low[:, half:], high[:, half:]], axis=1)
        out_ref[:, k * share : (k + 1) * share] = jnp.where(side == 0, even, odd).astype(jnp.bfloat16)
    lower = second_ref[:half].astype(jnp.float32)
    upper = second_ref[half:].astype(jnp.float32)
    out_ref[:, hidden // 2 :] = jnp.where(side == 0, lower, upper).astype(jnp.bfloat16)


def half_weights(w_first, w_second):
    depth, hidden = w_first.shape
    share, bottle = w_second.shape
    return pl.pallas_call(
        functools.partial(prep_kernel, share),
        out_shape=jax.ShapeDtypeStruct((depth, hidden // 2 + bottle), jnp.bfloat16),
        in_specs=[VMEM, VMEM],
        out_specs=VMEM,
        compiler_params=room(4),
        name="half_weights",
    )(w_first, w_second)


def spread_weights(x, size):
    far = [(hop(x, "dp", m), m) for m in range(4, size, 4)]
    pieces = [(x, [0])]
    if far:
        (near, mask), *far = far
        pieces = [(jnp.concatenate([x, near], axis=0), [0, mask])]
    pieces += [(y, [m]) for y, m in far]
    pieces += [(hop(y, "dp", 2), [m ^ 2 for m in ms]) for y, ms in pieces]
    pieces += [(hop(y, "dp", 1), [m ^ 1 for m in ms]) for y, ms in pieces]
    return pieces


def spread_protos(x, size, heads):
    bits = []
    bit = 4
    while bit < size:
        bits.append(bit)
        bit *= 2
    current, masks = x, [0]
    for bit in bits[:-1]:
        current = jnp.concatenate([current, hop(current, "dp", bit)], axis=0)
        masks = masks + [m ^ bit for m in masks]
    near = [(current, masks)]
    for bit in bits[-1:]:
        near.append((hop(current, "dp", bit), [m ^ bit for m in masks]))
    pieces = [(y, ms, 0) for y, ms in near]
    across = [(hop(y, "dp", 2), [m ^ 2 for m in ms], 0) for y, ms in near]
    side = [(hop(y, "head", 1), ms, 1) for y, ms in near] if heads > 1 else []
    corner = [
        (hop(y, "head", 1), ms, 1) if i % 2 == 0 else
        (hop(side[i][0], "dp", 2), ms, 1)
        for i, (y, ms, _) in enumerate(across[: len(side)])
    ]
    pieces = pieces + across + side + corner
    bit = 2
    while bit < heads:
        pieces += [(hop(y, "head", bit), ms, h ^ bit) for y, ms, h in pieces]
        bit *= 2
    return pieces + [(hop(y, "dp", 1), [m ^ 1 for m in ms], h) for y, ms, h in pieces]


def in_order(pieces, rows):
    blocks = [x[i * rows : (i + 1) * rows] for x, masks in pieces for i in range(len(masks))]
    masks = [m for _, ms in pieces for m in ms]
    place = jnp.asarray([masks.index(m) for m in range(len(masks))], jnp.int32)
    me = lax.axis_index("dp")
    order = jnp.take(place, jnp.arange(len(masks), dtype=jnp.int32) ^ me)
    return jnp.take(jnp.stack(blocks), order, axis=0).reshape(-1, blocks[0].shape[1])


def piece_copies(ref, masks, block, cols, target, place, sem):
    return [
        pltpu.make_async_copy(
            ref.at[pl.ds(i * block, block), cols], target.at[pl.ds(place(m), block), :], sem
        )
        for i, m in enumerate(masks)
    ]


def early_kernel(plan, block, own_ref, far_ref, *refs):
    piece_refs = refs[: len(plan)]
    own_out, far_out, first, sem = refs[len(plan) :]
    copies = []
    for ref, masks in zip(piece_refs, plan):
        copies += piece_copies(ref, masks, block, pl.ds(0, first.shape[1]), first, lambda m: m * block, sem)
    for copy in copies:
        copy.start()
    for copy in copies:
        copy.wait()
    depth, hidden = first.shape
    step = min(256, hidden)
    for i in range(hidden // step):
        cols = slice(i * step, (i + 1) * step)
        own_out[:, cols] = jnp.dot(own_ref[:, :depth], first[:, cols], preferred_element_type=jnp.float32)
        far_out[:, cols] = jnp.dot(far_ref[:, :depth], first[:, cols], preferred_element_type=jnp.float32)


def early_dot(own, far, pieces, block, hidden):
    plan = [masks for _, masks in pieces]
    depth = block * sum(len(masks) for masks in plan)
    part = jax.ShapeDtypeStruct((own.shape[0], hidden), jnp.float32)
    return pl.pallas_call(
        functools.partial(early_kernel, plan, block),
        out_shape=(part, part),
        in_specs=[VMEM, VMEM] + [HBM] * len(plan),
        out_specs=(VMEM, VMEM),
        scratch_shapes=[pltpu.VMEM((depth, hidden), jnp.bfloat16), pltpu.SemaphoreType.DMA],
        compiler_params=room(12),
        name="early_dot",
    )(own, far, *[x for x, _ in pieces])


def late_kernel(plan, block, begin, acc_ref, rows_ref, *refs):
    piece_refs = refs[: len(plan)]
    out_ref, first, second, sem, sem_second = refs[len(plan) :]
    me = lax.axis_index("dp")
    hidden, bottle = second.shape
    copies = []
    later = []
    for ref, masks in zip(piece_refs, plan):
        if masks[0] * block >= begin:
            copies += piece_copies(ref, masks, block, pl.ds(0, hidden), first, lambda m: m * block - begin, sem)
        later += piece_copies(
            ref, masks, block, pl.ds(hidden, bottle), second,
            lambda m: pl.multiple_of((me ^ m) * block, block), sem_second,
        )
    for copy in copies + later:
        copy.start()
    for copy in copies:
        copy.wait()
    step = min(256, hidden)
    total = jnp.zeros(out_ref.shape, jnp.float32)
    for i in range(hidden // step):
        cols = slice(i * step, (i + 1) * step)
        pre = acc_ref[:, cols] + jnp.dot(rows_ref[:, begin:], first[:, cols], preferred_element_type=jnp.float32)
        units = (0.5 * pre * (1.0 + lax.erf(pre * (0.5**0.5)))).astype(jnp.bfloat16)
        if i == 0:
            for copy in later:
                copy.wait()
        total += jnp.dot(units, second[cols, :], preferred_element_type=jnp.float32)
    out_ref[...] = total.astype(out_ref.dtype)


def late_layers(acc, rows, pieces, block, begin, bottle, dtype):
    plan = [masks for _, masks in pieces]
    depth = block * sum(len(masks) for masks in plan)
    hidden = acc.shape[1]
    return pl.pallas_call(
        functools.partial(late_kernel, plan, block, begin),
        out_shape=jax.ShapeDtypeStruct((rows.shape[0], bottle), dtype),
        in_specs=[VMEM, VMEM] + [HBM] * len(plan),
        out_specs=VMEM,
        scratch_shapes=[
            pltpu.VMEM((depth - begin, hidden), jnp.bfloat16),
            pltpu.VMEM((hidden, bottle), jnp.bfloat16),
            pltpu.SemaphoreType.DMA,
            pltpu.SemaphoreType.DMA,
        ],
        compiler_params=room(12),
    )(acc, rows, *[x for x, _ in pieces])


def norm_kernel(views, block, mine_ref, got_ref, mask_ref, normed_ref, sums_ref, whole):
    projected = mine_ref[...] + got_ref[...].astype(jnp.float32)
    scale = lax.rsqrt(jnp.sum(projected * projected, axis=-1, keepdims=True) + 1e-06)
    exact = (projected * scale).astype(jnp.bfloat16).astype(jnp.float32)
    whole[...] = exact
    by_mask(whole, lax.axis_index("dp") * block, normed_ref)
    bottle = exact.shape[1]
    view = lax.broadcasted_iota(jnp.int32, exact.shape, 0) % views
    lines = [jnp.sum(jnp.where(view == v, exact, 0.0), axis=0, keepdims=True) for v in range(views)]
    for v in range(views):
        count = jnp.sum(mask_ref[v].astype(jnp.float32), axis=1, keepdims=True)
        lines.append(jnp.broadcast_to(count, (1, bottle)))
    lines.append(jnp.zeros((sums_ref.shape[0] - len(lines), bottle), jnp.float32))
    sums_ref[...] = jnp.concatenate(lines, axis=0)


def norm_rows(mine, got, mask, views, block):
    return pl.pallas_call(
        functools.partial(norm_kernel, views, block),
        out_shape=(
            jax.ShapeDtypeStruct(mine.shape, jnp.bfloat16),
            jax.ShapeDtypeStruct((round_up(2 * views, 8), mine.shape[1]), jnp.float32),
        ),
        in_specs=[VMEM, VMEM, VMEM],
        out_specs=(VMEM, VMEM),
        scratch_shapes=[pltpu.VMEM(mine.shape, jnp.float32)],
        compiler_params=room(4),
        name="norm_rows",
    )(mine, got, mask)


def logits_kernel(plan, views, head_mask, normed_ref, center_ref, *refs):
    piece_refs = refs[: len(plan)]
    exps_ref, unit_ref = refs[len(plan) :]
    rows = normed_ref.shape[0]
    total = exps_ref.shape[1]
    block = piece_refs[0].shape[0] // len(plan[0])
    order = sorted((m, i, j) for i, masks in enumerate(plan) for j, m in enumerate(masks))
    begin = pl.multiple_of((lax.axis_index("head") ^ head_mask) * total, total)
    step = min(1024, total)
    view = lax.broadcasted_iota(jnp.int32, (rows, 1), 0) % views
    normed = normed_ref[...]
    for k in range(total // step):
        cols = slice(k * step, (k + 1) * step)
        parts = [piece_refs[i][j * block : (j + 1) * block, cols] for _, i, j in order]
        exact = jnp.concatenate(parts, axis=0).astype(jnp.float32)
        scale = lax.rsqrt(jnp.sum(exact * exact, axis=0, keepdims=True) + 1e-06)
        unit = (exact * scale).astype(jnp.bfloat16)
        unit_ref[:, cols] = unit
        logits = jnp.dot(normed, unit, preferred_element_type=jnp.float32)
        center = center_ref[:, pl.ds(begin + k * step, step)]
        shift = jnp.where(view == 0, center, 0.0)
        exps_ref[:, cols] = jnp.exp((logits - shift) * (1.0 / teacher_temp))


def logits_of(normed, center, pieces, views, head_mask):
    plan = [masks for _, masks in pieces]
    rows, bottle = normed.shape
    total = pieces[0][0].shape[1]
    return pl.pallas_call(
        functools.partial(logits_kernel, plan, views, head_mask),
        out_shape=(
            jax.ShapeDtypeStruct((rows, total), jnp.float32),
            jax.ShapeDtypeStruct((bottle, total), jnp.bfloat16),
        ),
        in_specs=[VMEM] * (2 + len(plan)),
        out_specs=(VMEM, VMEM),
        compiler_params=room(16),
    )(normed, center, *[x for x, _ in pieces])


def target_kernel(views, heads, block, capacity, sums_ref, mask_ref, center_ref, *refs):
    exps_refs = refs[:heads]
    unit_refs = refs[heads : 2 * heads]
    out_ref, new_ref, parts_ref, moved, ready, sem = refs[2 * heads :]
    rows, share = exps_refs[0].shape
    head = lax.axis_index("head")
    rest = sums_ref[0:views]
    lines = []
    for _ in range(SPLIT):
        line = rest.astype(jnp.bfloat16).astype(jnp.float32)
        lines.append(line)
        rest = rest - line
    lines.append(jnp.zeros((parts_ref.shape[0] - SPLIT * views, rest.shape[1]), jnp.float32))
    parts_ref[...] = jnp.concatenate(lines, axis=0)
    by_mask(parts_ref, lax.axis_index("dp") * block, moved)
    left = moved[...]
    counts = [sums_ref[views + v : views + v + 1, 0:1] for v in range(views)]
    step = min(1024, share)
    view = lax.broadcasted_iota(jnp.int32, (8, 1), 0) % views
    row_sums = jnp.zeros((rows, 1), jnp.float32)
    factors = []
    for h in range(heads):
        begin = pl.multiple_of((head ^ h) * share, share)
        for k in range(share // step):
            cols = slice(k * step, (k + 1) * step)
            sums = jnp.dot(left, unit_refs[h][:, cols], preferred_element_type=jnp.float32)
            center = center_ref[:, pl.ds(begin + k * step, step)]
            factor = jnp.ones((8, step), jnp.float32)
            for v in range(views):
                if v:
                    factor = jnp.where(view == v, jnp.exp(center * (-1.0 / teacher_temp)), factor)
                summed = sum(sums[p * views + v : p * views + v + 1] for p in range(SPLIT))
                center = center_momentum * center + (1.0 - center_momentum) * summed / counts[v]
            if h == 0:
                new_ref[:, cols] = center
            factors.append(factor)
            e = exps_refs[h][:, cols].reshape(rows // 8, 8, step) * factor[None]
            row_sums += jnp.sum(e.reshape(rows, step), axis=1, keepdims=True)
    line = lax.broadcasted_iota(jnp.int32, (rows, 1), 0)
    live = jnp.zeros((rows, 1), jnp.int32)
    for v in range(views):
        live = jnp.where(line % views == v, jnp.sum(mask_ref[v], axis=1, keepdims=True), live)
    gain = jnp.where(line // views < live, heads * share / row_sums, 0.0)
    outs = []
    for h in range(heads):
        begin = pl.multiple_of((head ^ h) * share, share)
        for k in range(share // step):
            cols = slice(k * step, (k + 1) * step)
            factor = factors[h * (share // step) + k]
            e = (exps_refs[h][:, cols].reshape(rows // 8, 8, step) * factor[None]).reshape(rows, step)
            scaled = (e * gain).astype(jnp.bfloat16)
            place = slice(h * share + k * step, h * share + (k + 1) * step)
            ready[:, :, place] = scaled.reshape(rows // views, views, step)[:capacity]
            copy = pltpu.make_async_copy(
                ready.at[:, :, place], out_ref.at[:, :, pl.ds(begin + k * step, step)], sem
            )
            copy.start()
            outs.append(copy)
    for copy in outs:
        copy.wait()


def targets_of(sums, mask, center, exps, units, views, block, capacity):
    heads = len(exps)
    _, share = exps[0].shape
    bottle = units[0].shape[0]
    targets, latest = pl.pallas_call(
        functools.partial(target_kernel, views, heads, block, capacity),
        out_shape=(
            jax.ShapeDtypeStruct((capacity, views, heads * share), jnp.bfloat16),
            jax.ShapeDtypeStruct((1, share), jnp.float32),
        ),
        in_specs=[VMEM] * (3 + 2 * heads),
        out_specs=(HBM, VMEM),
        scratch_shapes=[
            pltpu.VMEM((round_up(SPLIT * views, 16), bottle), jnp.float32),
            pltpu.VMEM((round_up(SPLIT * views, 16), bottle), jnp.bfloat16),
            pltpu.VMEM((capacity, views, heads * share), jnp.bfloat16),
            pltpu.SemaphoreType.DMA,
        ],
        compiler_params=room(20),
        name="targets",
    )(sums, mask, center, *exps, *units)
    return targets.transpose(1, 0, 2), latest


def program(features, patch_mask, w_first, w_second, proto_weight, center):
    n_dp = lax.axis_size("dp")
    n_head = lax.axis_size("head")
    views, images, patches, _ = features.shape
    capacity = images * (patches // 2)
    slots = round_up(capacity, 8)
    bottle = w_second.shape[1]
    mask = patch_mask.reshape(views, 1, images * patches)

    weight = half_weights(w_first, w_second)
    depth, hidden = w_first.shape
    rows = pack_rows(features, patch_mask, slots, depth)
    far_rows = hop(rows, "head", 1)
    weights = spread_weights(weight, n_dp)
    begin = (n_dp - 4 if n_dp > 8 else 0) * depth
    early = [piece for piece in weights if piece[1][0] * depth < begin]
    own_acc, far_acc = early_dot(rows, far_rows, early, depth, hidden // 2)
    theirs = late_layers(far_acc, far_rows, weights, depth, begin, bottle, jnp.bfloat16)
    mine = late_layers(own_acc, rows, weights, depth, begin, bottle, jnp.float32)
    block = proto_weight.shape[0]
    ordered = block % 16 != 0
    move = 0 if ordered else block
    normed, sums = norm_rows(mine, hop(theirs, "head", 1), mask, views, move)
    bits = [1]
    bit = 4
    while bit < n_dp:
        bits.append(bit)
        bit *= 2
    for bit in bits + [2]:
        sums = sums + hop(sums, "dp", bit)
    bit = 1
    while bit < n_head:
        sums = sums + hop(sums, "head", bit)
        bit *= 2

    by_head = {}
    for x, masks, h in spread_protos(proto_weight, n_dp, n_head):
        by_head.setdefault(h, []).append((x, masks))
    lanes = center.reshape(1, -1)
    exps = []
    units = []
    for h in range(n_head):
        pieces = [(in_order(by_head[h], block), [0])] if ordered else by_head[h]
        e, unit = logits_of(normed, lanes, pieces, views, h)
        exps.append(e)
        units.append(unit)
    targets, latest = targets_of(sums, mask, lanes, exps, units, views, move, capacity)
    return (targets, latest[0])


def solution(mesh):
    placed = (
        P(None, ("dp", "head"), None, None),
        P(None, ("dp", "head"), None),
        P("dp", None),
        P("dp", None),
        P("dp", "head"),
        P(),
    )
    return jax.shard_map(
        program,
        mesh=mesh,
        in_specs=placed,
        out_specs=(P(None, ("dp", "head"), None), P("head")),
        check_vma=False,
    )
```

```python
import functools

import jax
import jax.numpy as jnp
from jax import lax
from jax.experimental import pallas as pl
from jax.experimental.pallas import tpu as pltpu
from jax.sharding import PartitionSpec as P


teacher_temp = 0.04
center_momentum = 0.9
VMEM = pl.BlockSpec(memory_space=pltpu.VMEM)
HBM = pl.BlockSpec(memory_space=pl.ANY)
FIXED = pl.BlockSpec(memory_space=pltpu.HBM)
SPLIT = 3
MIB = 1024 * 1024
LANES = 128
EXTRA = 16
BASE = 256


def room(mib):
    return pltpu.CompilerParams(vmem_limit_bytes=mib * MIB)


def hop(x, axis, mask):
    size = lax.axis_size(axis)
    return lax.ppermute(x, axis, [(i, i ^ mask) for i in range(size)])


def round_up(n, m):
    return -(-n // m) * m


def by_mask(source, shift, out):
    low = lax.broadcasted_iota(jnp.int32, (LANES, LANES), 0)
    high = lax.broadcasted_iota(jnp.int32, (LANES, LANES), 1)
    within = (low == (high ^ (shift % LANES))).astype(jnp.float32).astype(jnp.bfloat16)
    for t in range(out.shape[1] // LANES):
        start = pl.multiple_of((t ^ (shift // LANES)) * LANES, LANES)
        tile = source[:, pl.ds(start, LANES)].astype(jnp.bfloat16)
        moved = jnp.dot(tile, within, preferred_element_type=jnp.float32)
        out[:, t * LANES : (t + 1) * LANES] = moved.astype(out.dtype)


def pack_kernel(depth, feats_hbm, mask_hbm, rows_ref, found, feats_ref, mask_ref, sems):
    feats_load = pltpu.make_async_copy(feats_hbm, feats_ref, sems.at[0])
    mask_load = pltpu.make_async_copy(mask_hbm, mask_ref, sems.at[1])
    feats_load.start()
    mask_load.start()
    patches, views, width = feats_ref.shape
    lines = patches * views
    patch = lax.broadcasted_iota(jnp.int32, (patches, lines), 0)
    line = lax.broadcasted_iota(jnp.int32, (patches, lines), 1)
    upto = (patch * views <= line).astype(jnp.float32).astype(jnp.bfloat16)
    same = (patch == line // views).astype(jnp.float32).astype(jnp.bfloat16)
    mask_load.wait()
    marks = jnp.concatenate([mask_ref[v].astype(jnp.float32) for v in range(views)], axis=0)
    marks = jnp.concatenate([marks, jnp.zeros((16 - views, patches), jnp.float32)], axis=0).astype(jnp.bfloat16)
    rank = jnp.dot(marks, upto, preferred_element_type=jnp.float32).astype(jnp.int32)
    hit = jnp.dot(marks, same, preferred_element_type=jnp.float32)
    at = lax.broadcasted_iota(jnp.int32, (1, lines), 1)
    key = jnp.full((1, lines), -1, jnp.int32)
    for v in range(views):
        wanted = (at % views == v) & (hit[v : v + 1] > 0.5)
        key = jnp.where(wanted, (rank[v : v + 1] - 1) * views + v, key)
    slot = lax.broadcasted_iota(jnp.int32, (found.shape[0], lines), 0)
    pick = (slot == key).astype(jnp.float32).astype(jnp.bfloat16)
    feats_load.wait()
    feats = feats_ref[...].reshape(lines, width)
    found[...] = jnp.dot(pick, feats, preferred_element_type=jnp.float32)
    by_mask(found, lax.axis_index("dp") * depth, rows_ref.at[: found.shape[0]])
    digits = []
    for v in range(views):
        count = jnp.sum(mask_ref[v], axis=1, keepdims=True)
        digits += [count % BASE, count // BASE]
    digits = [jnp.broadcast_to(d.astype(jnp.float32), (1, width)) for d in digits]
    digits.append(jnp.zeros((EXTRA - 2 * views, width), jnp.float32))
    rows_ref[found.shape[0] :] = jnp.concatenate(digits, axis=0).astype(jnp.bfloat16)


def pack_rows(features, patch_mask, slots, depth):
    views, images, patches, width = features.shape
    feats = features.reshape(views, images * patches, width).transpose(1, 0, 2)
    mask = patch_mask.reshape(views, 1, images * patches)
    return pl.pallas_call(
        functools.partial(pack_kernel, depth),
        out_shape=jax.ShapeDtypeStruct((views * slots + EXTRA, width), jnp.bfloat16),
        in_specs=[FIXED, FIXED],
        out_specs=VMEM,
        scratch_shapes=[
            pltpu.VMEM((views * slots, width), jnp.float32),
            pltpu.VMEM(feats.shape, feats.dtype),
            pltpu.VMEM(mask.shape, mask.dtype),
            pltpu.SemaphoreType.DMA((2,)),
        ],
        compiler_params=room(16),
        name="pack_rows",
    )(feats, mask)


def prep_kernel(share, first_hbm, second_hbm, out_ref, first_ref, second_ref, sems):
    side = lax.axis_index("head") % 2
    half = share // 2
    loads = [
        pltpu.make_async_copy(first_hbm, first_ref, sems.at[0]),
        pltpu.make_async_copy(second_hbm, second_ref, sems.at[1]),
    ]
    for load in loads:
        load.start()
    for load in loads:
        load.wait()
    hidden = first_ref.shape[1]
    for k in range(hidden // (2 * share)):
        low = first_ref[:, 2 * k * share : (2 * k + 1) * share].astype(jnp.float32)
        high = first_ref[:, (2 * k + 1) * share : (2 * k + 2) * share].astype(jnp.float32)
        even = jnp.concatenate([low[:, :half], high[:, :half]], axis=1)
        odd = jnp.concatenate([low[:, half:], high[:, half:]], axis=1)
        out_ref[:, k * share : (k + 1) * share] = jnp.where(side == 0, even, odd).astype(jnp.bfloat16)
    lower = second_ref[:half].astype(jnp.float32)
    upper = second_ref[half:].astype(jnp.float32)
    out_ref[:, hidden // 2 :] = jnp.where(side == 0, lower, upper).astype(jnp.bfloat16)


def half_weights(w_first, w_second):
    depth, hidden = w_first.shape
    share, bottle = w_second.shape
    return pl.pallas_call(
        functools.partial(prep_kernel, share),
        out_shape=jax.ShapeDtypeStruct((depth, hidden // 2 + bottle), jnp.bfloat16),
        in_specs=[FIXED, FIXED],
        out_specs=VMEM,
        scratch_shapes=[
            pltpu.VMEM(w_first.shape, w_first.dtype),
            pltpu.VMEM(w_second.shape, w_second.dtype),
            pltpu.SemaphoreType.DMA((2,)),
        ],
        compiler_params=room(4),
        name="half_weights",
    )(w_first, w_second)


def spread_weights(x, size):
    pieces = [(x, [0])] + [(hop(x, "dp", m), [m]) for m in range(4, size, 4)]
    pieces += [(hop(y, "dp", 2), [m ^ 2 for m in ms]) for y, ms in pieces]
    pieces += [(hop(y, "dp", 1), [m ^ 1 for m in ms]) for y, ms in pieces]
    return pieces


def spread_protos(x, size, heads):
    far = [(hop(x, "dp", m), m) for m in range(4, size, 4)]
    near = [(x, [0])]
    if far:
        (first, mask), *far = far
        near = [(jnp.concatenate([x, first], axis=0), [0, mask])]
    near += [(y, [m]) for y, m in far]
    pieces = [(y, ms, 0) for y, ms in near]
    across = [(hop(y, "dp", 2), [m ^ 2 for m in ms], 0) for y, ms in near]
    side = [(hop(y, "head", 1), ms, 1) for y, ms in near] if heads > 1 else []
    corner = [
        (hop(y, "head", 1), ms, 1) if i == 0 else
        (hop(side[i][0], "dp", 2), ms, 1)
        for i, (y, ms, _) in enumerate(across[: len(side)])
    ]
    pieces = pieces + across + side + corner
    bit = 2
    while bit < heads:
        pieces += [(hop(y, "head", bit), ms, h ^ bit) for y, ms, h in pieces]
        bit *= 2
    return pieces + [(hop(y, "dp", 1), [m ^ 1 for m in ms], h) for y, ms, h in pieces]


def in_order(pieces, rows):
    blocks = [x[i * rows : (i + 1) * rows] for x, masks in pieces for i in range(len(masks))]
    masks = [m for _, ms in pieces for m in ms]
    place = jnp.asarray([masks.index(m) for m in range(len(masks))], jnp.int32)
    me = lax.axis_index("dp")
    order = jnp.take(place, jnp.arange(len(masks), dtype=jnp.int32) ^ me)
    return jnp.take(jnp.stack(blocks), order, axis=0).reshape(-1, blocks[0].shape[1])


def piece_copies(ref, masks, block, cols, target, place, sem):
    return [
        pltpu.make_async_copy(
            ref.at[pl.ds(i * block, block), cols], target.at[pl.ds(place(m), block), :], sem
        )
        for i, m in enumerate(masks)
    ]


def early_kernel(plan, block, own_ref, far_ref, *refs):
    piece_refs = refs[: len(plan)]
    own_out, far_out, first, sem = refs[len(plan) :]
    copies = []
    for ref, masks in zip(piece_refs, plan):
        copies += piece_copies(ref, masks, block, pl.ds(0, first.shape[1]), first, lambda m: m * block, sem)
    for copy in copies:
        copy.start()
    for copy in copies:
        copy.wait()
    depth, hidden = first.shape
    rows = own_out.shape[0]
    step = min(256, hidden)
    for i in range(hidden // step):
        cols = slice(i * step, (i + 1) * step)
        own_out[:, cols] = jnp.dot(own_ref[:rows, :depth], first[:, cols], preferred_element_type=jnp.float32)
        far_out[:, cols] = jnp.dot(far_ref[:rows, :depth], first[:, cols], preferred_element_type=jnp.float32)


def early_dot(own, far, pieces, block, hidden):
    plan = [masks for _, masks in pieces]
    depth = block * sum(len(masks) for masks in plan)
    part = jax.ShapeDtypeStruct((own.shape[0] - EXTRA, hidden), jnp.float32)
    return pl.pallas_call(
        functools.partial(early_kernel, plan, block),
        out_shape=(part, part),
        in_specs=[VMEM, VMEM] + [HBM] * len(plan),
        out_specs=(VMEM, VMEM),
        scratch_shapes=[pltpu.VMEM((depth, hidden), jnp.bfloat16), pltpu.SemaphoreType.DMA],
        compiler_params=room(12),
        name="early_dot",
    )(own, far, *[x for x, _ in pieces])


def late_kernel(plan, block, begin, own_acc, far_acc, own_ref, far_ref, *refs):
    piece_refs = refs[: len(plan)]
    both_ref, sent_ref, first, second, sem, sem_second = refs[len(plan) :]
    me = lax.axis_index("dp")
    hidden, bottle = second.shape
    copies = []
    later = []
    for ref, masks in zip(piece_refs, plan):
        if masks[0] * block >= begin:
            copies += piece_copies(ref, masks, block, pl.ds(0, hidden), first, lambda m: m * block - begin, sem)
        later += piece_copies(
            ref, masks, block, pl.ds(hidden, bottle), second,
            lambda m: pl.multiple_of((me ^ m) * block, block), sem_second,
        )
    for copy in copies + later:
        copy.start()
    for copy in copies:
        copy.wait()
    count = own_acc.shape[0]
    step = min(256, hidden)
    totals = [jnp.zeros((count, bottle), jnp.float32)] * 2
    for i in range(hidden // step):
        cols = slice(i * step, (i + 1) * step)
        for k, (acc, rows) in enumerate(((own_acc, own_ref), (far_acc, far_ref))):
            more = jnp.dot(rows[:count, begin:], first[:, cols], preferred_element_type=jnp.float32)
            pre = acc[:, cols] + more
            units = (0.5 * pre * (1.0 + lax.erf(pre * (0.5**0.5)))).astype(jnp.bfloat16)
            if i + k == 0:
                for copy in later:
                    copy.wait()
            totals[k] += jnp.dot(units, second[cols, :], preferred_element_type=jnp.float32)
    both = jnp.concatenate(totals, axis=0)
    both_ref[...] = both
    sent_ref[...] = both.astype(jnp.bfloat16)


def late_layers(own_acc, far_acc, own, far, pieces, block, begin, bottle):
    plan = [masks for _, masks in pieces]
    depth = block * sum(len(masks) for masks in plan)
    count, hidden = own_acc.shape
    return pl.pallas_call(
        functools.partial(late_kernel, plan, block, begin),
        out_shape=(
            jax.ShapeDtypeStruct((2 * count, bottle), jnp.float32),
            jax.ShapeDtypeStruct((2 * count, bottle), jnp.bfloat16),
        ),
        in_specs=[VMEM] * 4 + [HBM] * len(plan),
        out_specs=(VMEM, VMEM),
        scratch_shapes=[
            pltpu.VMEM((depth - begin, hidden), jnp.bfloat16),
            pltpu.VMEM((hidden, bottle), jnp.bfloat16),
            pltpu.SemaphoreType.DMA,
            pltpu.SemaphoreType.DMA,
        ],
        compiler_params=room(16),
        name="late_layers",
    )(own_acc, far_acc, own, far, *[x for x, _ in pieces])


def norm_kernel(views, block, both_ref, got_ref, own_ref, far_ref, normed_ref, sums_ref, whole):
    count = normed_ref.shape[0]
    projected = both_ref[...] + jnp.concatenate([got_ref[count:], got_ref[:count]], axis=0).astype(jnp.float32)
    scale = lax.rsqrt(jnp.sum(projected * projected, axis=-1, keepdims=True) + 1e-06)
    exact = (projected * scale).astype(jnp.bfloat16).astype(jnp.float32)
    whole[...] = exact[:count]
    by_mask(whole, lax.axis_index("dp") * block, normed_ref)
    bottle = exact.shape[1]
    view = lax.broadcasted_iota(jnp.int32, exact.shape, 0) % views
    lines = [jnp.sum(jnp.where(view == v, exact, 0.0), axis=0, keepdims=True) for v in range(views)]
    digits = own_ref[count:, :bottle].astype(jnp.float32) + far_ref[count:, :bottle].astype(jnp.float32)
    lines += [digits[2 * v : 2 * v + 1] + BASE * digits[2 * v + 1 : 2 * v + 2] for v in range(views)]
    lines.append(jnp.zeros((sums_ref.shape[0] - len(lines), bottle), jnp.float32))
    sums_ref[...] = jnp.concatenate(lines, axis=0)


def norm_rows(both, got, own, far, views, block):
    count = both.shape[0] // 2
    bottle = both.shape[1]
    return pl.pallas_call(
        functools.partial(norm_kernel, views, block),
        out_shape=(
            jax.ShapeDtypeStruct((count, bottle), jnp.bfloat16),
            jax.ShapeDtypeStruct((round_up(2 * views, 8), bottle), jnp.float32),
        ),
        in_specs=[VMEM] * 4,
        out_specs=(VMEM, VMEM),
        scratch_shapes=[pltpu.VMEM((count, bottle), jnp.float32)],
        compiler_params=room(6),
        name="norm_rows",
    )(both, got, own, far)


def logits_kernel(plan, views, head_mask, normed_ref, center_ref, *refs):
    piece_refs = refs[: len(plan)]
    exps_ref, unit_ref = refs[len(plan) :]
    rows = normed_ref.shape[0]
    total = exps_ref.shape[1]
    block = piece_refs[0].shape[0] // len(plan[0])
    order = sorted((m, i, j) for i, masks in enumerate(plan) for j, m in enumerate(masks))
    begin = pl.multiple_of((lax.axis_index("head") ^ head_mask) * total, total)
    step = min(1024, total)
    view = lax.broadcasted_iota(jnp.int32, (rows, 1), 0) % views
    normed = normed_ref[...]
    for k in range(total // step):
        cols = slice(k * step, (k + 1) * step)
        parts = [piece_refs[i][j * block : (j + 1) * block, cols] for _, i, j in order]
        exact = jnp.concatenate(parts, axis=0).astype(jnp.float32)
        scale = lax.rsqrt(jnp.sum(exact * exact, axis=0, keepdims=True) + 1e-06)
        unit = (exact * scale).astype(jnp.bfloat16)
        unit_ref[:, cols] = unit
        logits = jnp.dot(normed, unit, preferred_element_type=jnp.float32)
        center = center_ref[:, pl.ds(begin + k * step, step)]
        shift = jnp.where(view == 0, center, 0.0)
        exps_ref[:, cols] = jnp.exp((logits - shift) * (1.0 / teacher_temp))


def logits_of(normed, center, pieces, views, head_mask):
    plan = [masks for _, masks in pieces]
    rows, bottle = normed.shape
    total = pieces[0][0].shape[1]
    return pl.pallas_call(
        functools.partial(logits_kernel, plan, views, head_mask),
        out_shape=(
            jax.ShapeDtypeStruct((rows, total), jnp.float32),
            jax.ShapeDtypeStruct((bottle, total), jnp.bfloat16),
        ),
        in_specs=[VMEM] * (2 + len(plan)),
        out_specs=(VMEM, VMEM),
        compiler_params=room(16),
    )(normed, center, *[x for x, _ in pieces])


def target_kernel(views, heads, block, capacity, sums_ref, mask_ref, center_ref, *refs):
    exps_refs = refs[:heads]
    unit_refs = refs[heads : 2 * heads]
    out_ref, new_ref, parts_ref, moved, factors, ready, sem = refs[2 * heads :]
    rows, share = exps_refs[0].shape
    head = lax.axis_index("head")
    rest = sums_ref[0:views]
    lines = []
    for _ in range(SPLIT):
        line = rest.astype(jnp.bfloat16).astype(jnp.float32)
        lines.append(line)
        rest = rest - line
    lines.append(jnp.zeros((parts_ref.shape[0] - SPLIT * views, rest.shape[1]), jnp.float32))
    parts_ref[...] = jnp.concatenate(lines, axis=0)
    by_mask(parts_ref, lax.axis_index("dp") * block, moved)
    left = moved[...]
    counts = [sums_ref[views + v : views + v + 1, 0:1] for v in range(views)]
    step = min(1024, share)
    view = lax.broadcasted_iota(jnp.int32, (8, 1), 0) % views
    row_sums = jnp.zeros((rows, 1), jnp.float32)
    for h in range(heads):
        begin = pl.multiple_of((head ^ h) * share, share)
        for k in range(share // step):
            cols = slice(k * step, (k + 1) * step)
            sums = jnp.dot(left, unit_refs[h][:, cols], preferred_element_type=jnp.float32)
            center = center_ref[:, pl.ds(begin + k * step, step)]
            factor = jnp.ones((8, step), jnp.float32)
            for v in range(views):
                if v:
                    factor = jnp.where(view == v, jnp.exp(center * (-1.0 / teacher_temp)), factor)
                summed = sum(sums[p * views + v : p * views + v + 1] for p in range(SPLIT))
                center = center_momentum * center + (1.0 - center_momentum) * summed / counts[v]
            if h == 0:
                new_ref[:, cols] = center
            factors[h, :, cols] = factor
            e = exps_refs[h][:, cols].reshape(rows // 8, 8, step) * factor[None]
            row_sums += jnp.sum(e.reshape(rows, step), axis=1, keepdims=True)
    line = lax.broadcasted_iota(jnp.int32, (rows, 1), 0)
    live = jnp.zeros((rows, 1), jnp.int32)
    for v in range(views):
        live = jnp.where(line % views == v, jnp.sum(mask_ref[v], axis=1, keepdims=True), live)
    gain = jnp.where(line // views < live, heads * share / row_sums, 0.0)
    outs = []
    for top in range(0, rows, 16):
        for h in range(heads):
            begin = pl.multiple_of((head ^ h) * share, share)
            e = exps_refs[h][top : top + 16].reshape(2, 8, share) * factors[h][None]
            ready[top : top + 16, pl.ds(begin, share)] = (
                e.reshape(16, share) * gain[top : top + 16]
            ).astype(jnp.bfloat16)
        for slot in range(top // views, min((top + 16) // views, capacity)):
            copy = pltpu.make_async_copy(ready.at[pl.ds(slot * views, views)], out_ref.at[slot], sem)
            copy.start()
            outs.append(copy)
    for copy in outs:
        copy.wait()


def targets_of(sums, mask, center, exps, units, views, block, capacity):
    heads = len(exps)
    rows, share = exps[0].shape
    bottle = units[0].shape[0]
    targets, latest = pl.pallas_call(
        functools.partial(target_kernel, views, heads, block, capacity),
        out_shape=(
            jax.ShapeDtypeStruct((capacity, views, heads * share), jnp.bfloat16),
            jax.ShapeDtypeStruct((1, share), jnp.float32),
        ),
        in_specs=[VMEM] * (3 + 2 * heads),
        out_specs=(HBM, VMEM),
        scratch_shapes=[
            pltpu.VMEM((round_up(SPLIT * views, 16), bottle), jnp.float32),
            pltpu.VMEM((round_up(SPLIT * views, 16), bottle), jnp.bfloat16),
            pltpu.VMEM((heads, 8, share), jnp.float32),
            pltpu.VMEM((rows, heads * share), jnp.bfloat16),
            pltpu.SemaphoreType.DMA,
        ],
        compiler_params=room(20),
        name="targets",
    )(sums, mask, center, *exps, *units)
    return targets.transpose(1, 0, 2), latest


def program(features, patch_mask, w_first, w_second, proto_weight, center):
    n_dp = lax.axis_size("dp")
    n_head = lax.axis_size("head")
    views, images, patches, _ = features.shape
    capacity = images * (patches // 2)
    slots = round_up(capacity, 8)
    bottle = w_second.shape[1]
    mask = patch_mask.reshape(views, 1, images * patches)
    weight = half_weights(w_first, w_second)
    depth, hidden = w_first.shape
    rows = pack_rows(features, patch_mask, slots, depth)
    far_rows = hop(rows, "head", 1)
    weights = spread_weights(weight, n_dp)
    begin = (n_dp - 4 if n_dp > 8 else 0) * depth
    early = [piece for piece in weights if piece[1][0] * depth < begin]
    own_acc, far_acc = early_dot(rows, far_rows, early, depth, hidden // 2)
    both, sent = late_layers(own_acc, far_acc, rows, far_rows, weights, depth, begin, bottle)
    block = proto_weight.shape[0]
    ordered = block % 16 != 0
    move = 0 if ordered else block
    normed, sums = norm_rows(both, hop(sent, "head", 1), rows, far_rows, views, move)
    hops = [("dp", 1)]
    bit = 4
    while bit < n_dp:
        hops.append(("dp", bit))
        bit *= 2
    hops.append(("dp", 2))
    bit = 2
    while bit < n_head:
        hops.append(("head", bit))
        bit *= 2
    for axis, bit in hops:
        sums = sums + hop(sums, axis, bit)

    by_head = {}
    for x, masks, h in spread_protos(proto_weight, n_dp, n_head):
        by_head.setdefault(h, []).append((x, masks))
    lanes = center.reshape(1, -1)
    exps = []
    units = []
    for h in range(n_head):
        pieces = [(in_order(by_head[h], block), [0])] if ordered else by_head[h]
        e, unit = logits_of(normed, lanes, pieces, views, h)
        exps.append(e)
        units.append(unit)
    targets, latest = targets_of(sums, mask, lanes, exps, units, views, move, capacity)
    return (targets, latest[0])


def solution(mesh):
    placed = (
        P(None, ("dp", "head"), None, None),
        P(None, ("dp", "head"), None),
        P("dp", None),
        P("dp", None),
        P("dp", "head"),
        P(),
    )
    return jax.shard_map(
        program,
        mesh=mesh,
        in_specs=placed,
        out_specs=(P(None, ("dp", "head"), None), P("head")),
        check_vma=False,
    )
```
